32 devices in a mesh: dp: 4 (over z), task: 4 (over y, x), mp: 2 (over core).
Axes of the slice: x: 2, y: 2, z: 4, core: 2. Of those that a mesh axis runs over, the one named last changes fastest.
Arguments:
- deltas: bfloat16 [4, 2, 128, 28672], P('task', None, 'dp', 'mp'), may hold values from -3.984375 to 3.984375, as said below
- keep_blocks: int32 [4, 2, 1], P('task'), may hold values 0 or 1
- base_weights: bfloat16 [2, 128, 28672], P(None, 'dp', 'mp'), may hold values from -6 to 6
Outputs:
- merged: float32 [2, 128, 28672], P(None, 'dp', 'mp')
The draws below stay inside these ranges and needn't reach their ends.
Inputs may be any that keep to these rules, and one draw needn't show every extreme that they name: `deltas`: every entry is a whole multiple of 1/64.
All inputs are finite; a program needn't handle non-finite values. No bound on the sum of `keep_blocks` on one device may be relied on, other than what follows from the above.
Results may differ from the reference program's by a relative error of at most 0.0003.
Values may be sent and summed in bfloat16 or wider, within the bound.
No kernel may reach another device: no remote copies, remote signals or barrier semaphores. Data moves between devices by JAX's collectives and lax.ppermute only.
A program may use at most 128 MiB of HBM per device.

```python
import jax
import jax.numpy as jnp

FF = 28672
BLOCK = 128
ROWS = 128
BLOCKS = 1
TASKS = 4


def draw_deltas(key, part):
    shape = (TASKS, 2, ROWS, FF)
    first_key, second_key = jax.random.split(jax.random.fold_in(key, 17))
    level = jax.random.randint(first_key, shape, -128, 129) + jax.random.randint(second_key, shape, -127, 128)
    return (level.astype(jnp.float32) / 64.0).astype(jnp.bfloat16)


def place_ends(entries, stream_key, least, high):
    index_at = [jax.random.randint(jax.random.fold_in(stream_key, axis), (), 0, length) for axis, length in enumerate(entries.shape)]
    widest = entries.shape.index(max(entries.shape))
    neighbour = index_at[:widest] + [(index_at[widest] + 1) % entries.shape[widest]] + index_at[widest + 1:]
    return entries.at[tuple(index_at)].set(least).at[tuple(neighbour)].set(high)


def block_levels(own_key, shape, pieces, least, high):
    def one(position, parts):
        heights = jax.random.uniform(jax.random.fold_in(jax.random.fold_in(own_key, 6), position), (parts,), jnp.float32, least / len(pieces), high / len(pieces))
        return jnp.repeat(jnp.exp(heights), shape[position] // parts).reshape((-1,) + (1,) * (len(shape) - position - 1))

    loudness = one(*pieces[0])
    for cut in pieces[1:]:
        loudness = loudness * one(*cut)
    return loudness


def centred(stream_key, extent, deviation, most, cuts=(), dtype=jnp.bfloat16):
    loudness = block_levels(stream_key, extent, cuts, -0.22, 0.18) if cuts else 1.0
    values = jax.random.normal(stream_key, extent, jnp.float32) * deviation * loudness
    return jnp.minimum(jnp.maximum(values, -most), most).astype(dtype)


def setup_inputs(seed: int = 0) -> dict:
    keys = jax.random.split(jax.random.key(seed), 4)
    deltas = draw_deltas(jax.random.fold_in(keys[3], 71), 0)
    keep_blocks = place_ends((jax.random.randint(keys[1], (TASKS, 2, BLOCKS), 0, 2) < 1).astype(jnp.int32), jax.random.fold_in(keys[1], 1), 0, 1)
    base_weights = centred(keys[2], (2, ROWS, FF), 1.0, 6.0, ((1, 4), (2, 2)))
    return dict(deltas=deltas, keep_blocks=keep_blocks, base_weights=base_weights)


def reference(deltas, keep_blocks, base_weights):
    row_keep = jnp.repeat(keep_blocks, BLOCK, axis=2).astype(jnp.float32)
    shape = base_weights.shape
    upward = jnp.zeros(shape, jnp.float32)
    downward = jnp.zeros(shape, jnp.float32)
    up_count = jnp.zeros(shape, jnp.float32)
    down_count = jnp.zeros(shape, jnp.float32)
    for which in range(TASKS):
        trimmed = deltas[which].astype(jnp.float32) * row_keep[which][:, :, None]
        upward = upward + jnp.maximum(trimmed, 0.0)
        downward = downward + jnp.minimum(trimmed, 0.0)
        up_count = up_count + (trimmed > 0).astype(jnp.float32)
        down_count = down_count + (trimmed < 0).astype(jnp.float32)
    elected = jnp.sign(upward + downward)
    upper_mean = upward / jnp.maximum(up_count, 1.0)
    lower_mean = downward / jnp.maximum(down_count, 1.0)
    agreed = jnp.where(elected > 0, upper_mean, jnp.where(elected < 0, lower_mean, 0.0))
    return base_weights.astype(jnp.float32) + agreed
```

```python
import math

import jax
import jax.numpy as jnp
from jax import lax
from jax.sharding import PartitionSpec as P

BLOCK = 128
STEPS = 64
LEVELS = 255


def total(parts):
    out = parts[0]
    for part in parts[1:]:
        out = out + part
    return out


def elect(parts):
    wide = [part.astype(jnp.float32) for part in parts]
    upward = total([jnp.maximum(w, 0.0) for w in wide])
    downward = total([jnp.minimum(w, 0.0) for w in wide])
    up_count = total([(w > 0).astype(jnp.float32) for w in wide])
    down_count = total([(w < 0).astype(jnp.float32) for w in wide])
    balance = upward + downward
    side = jnp.where(balance > 0, upward, downward)
    count = jnp.where(balance > 0, up_count, down_count)
    return jnp.where(balance == 0, 0.0, side), jnp.maximum(count, 1.0)


def kept(keep_blocks, rows):
    row_start = lax.axis_index("dp") * rows
    if BLOCK % rows == 0:
        return lax.dynamic_slice_in_dim(keep_blocks, row_start // BLOCK, 1, 1)
    blocks = (row_start + jnp.arange(rows, dtype=jnp.int32)) // BLOCK
    return jnp.take(keep_blocks, blocks, axis=1)


def on_any_group(deltas, keep_blocks, base_weights):
    n = lax.axis_size("task")
    _, projections, rows, width = deltas.shape
    keep = kept(keep_blocks[0], rows)
    trimmed = jnp.where(keep[:, :, None] != 0, deltas[0], jnp.zeros((), deltas.dtype))
    split = trimmed.reshape(projections, n, rows // n, width).swapaxes(0, 1)
    arrived = lax.all_to_all(split, "task", split_axis=0, concat_axis=0, tiled=True)
    side, count = elect([arrived[i] for i in range(n)])
    agreed = lax.all_gather(side / count, "task", axis=1, tiled=True)
    return base_weights.astype(jnp.float32) + agreed


def on_square(deltas, keep_blocks, base_weights):
    n = 4
    me = lax.axis_index("task")
    _, projections, rows, width = deltas.shape
    share, half = rows // n, width // 2
    unit = STEPS * math.lcm(*range(1, n + 1))
    keep = kept(keep_blocks[0], rows)

    def permute(x, mask):
        return lax.ppermute(x, "task", [(i, i ^ mask) for i in range(n)])

    columns = []
    for p in range(projections):
        trimmed = jnp.where(keep[p][:, None] != 0, deltas[0, p], jnp.zeros((), deltas.dtype))
        pieces = trimmed.reshape(n, share, width)
        piece = [lax.dynamic_index_in_dim(pieces, me ^ m, 0, False) for m in range(n)]
        columns.append([piece[0]] + [permute(piece[m], m) for m in range(1, n)])
    outs = []
    for p in range(projections):
        side, count = elect(columns[p])
        code = jnp.round(side * (unit / count)).astype(jnp.int16)
        beside, above = permute(code, 1), permute(code, 2)
        across = jnp.concatenate(
            [permute(beside[:, :half], 2), permute(above[:, half:], 1)], 1
        )
        held = [code, beside, above, across]
        odd, high = (me & 1) == 1, (me & 2) == 2
        swapped = [jnp.where(odd, held[i ^ 1], held[i]) for i in range(n)]
        ordered = [jnp.where(high, swapped[i ^ 2], swapped[i]) for i in range(n)]
        agreed = jnp.concatenate(ordered, 0).astype(jnp.float32) * (1.0 / unit)
        outs.append(base_weights[p].astype(jnp.float32) + agreed)
    return jnp.stack(outs)


def on_device(deltas, keep_blocks, base_weights):
    n = lax.axis_size("task")
    codes = LEVELS * math.lcm(*range(1, n + 1))
    if n == 4 and deltas.shape[2] % n == 0 and codes < 2**15:
        return on_square(deltas, keep_blocks, base_weights)
    return on_any_group(deltas, keep_blocks, base_weights)


def solution(mesh):
    in_specs = (P("task", None, "dp", "mp"), P("task", None, None), P(None, "dp", "mp"))
    out_specs = P(None, "dp", "mp")
    return jax.shard_map(
        on_device, mesh=mesh, in_specs=in_specs, out_specs=out_specs, check_vma=False
    )
```

```python
import functools
import math

import jax
import jax.numpy as jnp
from jax import lax
from jax.experimental import pallas as pl
from jax.experimental.pallas import tpu as pltpu
from jax.sharding import PartitionSpec as P


BLOCK = 128
STEPS = 64
LEVELS = 255
LANES = 128
TASKS = 4
UNIT = math.lcm(*range(1, TASKS + 1))
HBM = pl.BlockSpec(memory_space=pltpu.HBM)
VMEM = pl.BlockSpec(memory_space=pltpu.VMEM)


def params(**more):
    return pltpu.CompilerParams(vmem_limit_bytes=8 * 2**20, **more)


def hops(core):
    first = 1 + core % 2
    return 0, first, 3 - first, 3


def total(parts):
    out = parts[0]
    for part in parts[1:]:
        out = out + part
    return out


def split_kernel(p, keep_ref, pieces_ref, *rest):
    outs, (keep, sems, keep_sem) = rest[:TASKS], rest[TASKS:]
    me = lax.axis_index("task")
    block = 0
    if keep_ref.shape[0] > 1:
        block = lax.axis_index("dp") * (TASKS * outs[0].shape[0]) // BLOCK
    flag = pltpu.make_async_copy(keep_ref, keep, keep_sem)
    copies = [
        pltpu.make_async_copy(pieces_ref.at[p, me ^ mask], outs[k], sems.at[k])
        for k, mask in enumerate(hops(lax.axis_index("mp")))
    ]
    flag.start()
    for copy in copies:
        copy.start()
    flag.wait()
    for copy in copies:
        copy.wait()

    @pl.when(keep[block, p] == 0)
    def _():
        for out in outs:
            out[...] = jnp.zeros_like(out)


def split(keep, pieces, p):
    _, _, share, width = pieces.shape
    return pl.pallas_call(
        functools.partial(split_kernel, p),
        out_shape=[pltpu.VMEM((share, width), pieces.dtype)] * TASKS,
        in_specs=[HBM, HBM],
        out_specs=[VMEM] * TASKS,
        scratch_shapes=[
            pltpu.SMEM(keep.shape, jnp.int32),
            pltpu.SemaphoreType.DMA((TASKS,)),
            pltpu.SemaphoreType.DMA,
        ],
        compiler_params=params(),
    )(keep, pieces)


def elect_kernel(*refs):
    *parts, code_ref = refs

    def step(j, _):
        at = (slice(None), pl.ds(pl.multiple_of(j * LANES, LANES), LANES))
        wide = [part[at].astype(jnp.float32) for part in parts]
        balance = total(wide)
        sign = jnp.where(balance > 0, 1.0, jnp.where(balance < 0, -1.0, 0.0))
        toward = sign * STEPS
        agreeing = [jnp.maximum(w * toward, 0.0) for w in wide]
        count = total([jnp.minimum(a, 1.0) for a in agreeing])
        scale = jnp.full_like(count, UNIT)
        for c in range(2, TASKS + 1):
            scale = jnp.where(count == c, float(UNIT // c), scale)
        code = total(agreeing) * (scale * sign)
        code_ref[at] = code.astype(jnp.int32).astype(jnp.int16)
        return 0

    lax.fori_loop(0, code_ref.shape[1] // LANES, step, 0, unroll=8)


def elect(parts):
    share, width = parts[0].shape
    return pl.pallas_call(
        elect_kernel,
        out_shape=pltpu.VMEM((share, width), jnp.int16),
        in_specs=[VMEM] * TASKS,
        out_specs=VMEM,
        compiler_params=params(),
    )(*parts)


def merge_kernel(places, base_ref, *rest):
    codes = rest[: len(places)]
    out_ref, staged, sems = rest[-3:]
    me, masks = lax.axis_index("task"), hops(lax.axis_index("mp"))
    copies = []
    for k, (p, m, first) in enumerate(places):
        width = codes[k].shape[1]

        def step(j, _, k=k, p=p, m=m, first=first):
            at = pl.ds(pl.multiple_of(j * LANES, LANES), LANES)
            source = pl.ds(pl.multiple_of(first + j * LANES, LANES), LANES)
            mean = codes[k][:, at].astype(jnp.int32).astype(jnp.float32)
            base = base_ref[p, me ^ masks[m], :, source].astype(jnp.float32)
            staged[k, :, at] = base + mean * (1.0 / (STEPS * UNIT))
            return 0

        lax.fori_loop(0, width // LANES, step, 0, unroll=8)
        copies.append(
            pltpu.make_async_copy(
                staged.at[k, :, pl.ds(0, width)],
                out_ref.at[p, me ^ masks[m], :, pl.ds(first, width)],
                sems.at[k],
            )
        )
        copies[-1].start()
    for copy in copies:
        copy.wait()


def merge(base, codes, places, so_far):
    share, width = codes[0].shape[0], max(c.shape[1] for c in codes)
    extra, alias = ([], {}) if so_far is None else ([so_far], {1 + len(codes): 0})
    return merge_call(base, codes, places, extra, alias, share, width)


def merge_call(base, codes, places, extra, alias, share, width):
    return pl.pallas_call(
        functools.partial(merge_kernel, places),
        out_shape=pltpu.HBM(base.shape, jnp.float32),
        in_specs=[VMEM] + [VMEM] * len(codes) + [HBM] * len(extra),
        out_specs=HBM,
        scratch_shapes=[
            pltpu.VMEM((len(codes), share, width), jnp.float32),
            pltpu.SemaphoreType.DMA((len(codes),)),
        ],
        input_output_aliases=alias,
        compiler_params=params(),
    )(base, *codes, *extra)


def square_body(deltas, keep_blocks, base_weights):
    _, projections, rows, width = deltas.shape
    share, half = rows // TASKS, width // 2
    pieces = deltas.reshape(projections, TASKS, share, width)
    base = base_weights.reshape(projections, TASKS, share, width)
    keep = keep_blocks.transpose(0, 2, 1).reshape(-1, projections)
    keep, pieces = (pltpu.with_memory_space_constraint(a, pltpu.HBM) for a in (keep, pieces))

    cores = lax.axis_size("mp")

    def permute(x, hop):
        ends = [(i, i ^ hops(c)[hop], c) for i in range(TASKS) for c in range(cores)]
        pairs = [(i * cores + c, j * cores + c) for i, j, c in ends]
        return lax.ppermute(x, ("task", "mp"), pairs)

    parts = []
    for p in range(projections):
        own, *others = split(keep, pieces, p)
        parts.append([own] + [permute(x, m) for m, x in enumerate(others, 1)])
    code, first, second = [], [], []
    for p in range(projections):
        code.append(elect(parts[p]))
        first.append(permute(code[p], 1))
        second.append(permute(code[p], 2))
    left = [permute(first[p][:, :half], 2) for p in range(projections)]
    right = [permute(second[p][:, half:], 1) for p in range(projections)]
    merged = None
    for p in range(projections):
        near = [(p, 0, 0), (p, 1, 0), (p, 2, 0)]
        merged = merge(base, [code[p], first[p], second[p]], near, merged)
        far = [(p, 3, 0), (p, 3, half)]
        merged = merge(base, [left[p], right[p]], far, merged)
    return merged.reshape(base_weights.shape)


def on_any_group(deltas, keep_blocks, base_weights):
    n = lax.axis_size("task")
    _, projections, rows, width = deltas.shape
    row_start = lax.axis_index("dp") * rows
    blocks = (row_start + jnp.arange(rows, dtype=jnp.int32)) // BLOCK
    keep = jnp.take(keep_blocks[0], blocks, axis=1)
    trimmed = jnp.where(keep[:, :, None] != 0, deltas[0], jnp.zeros((), deltas.dtype))
    split_rows = trimmed.reshape(projections, n, rows // n, width).swapaxes(0, 1)
    arrived = lax.all_to_all(split_rows, "task", split_axis=0, concat_axis=0, tiled=True)
    wide = [arrived[i].astype(jnp.float32) for i in range(n)]
    upward = total([jnp.maximum(w, 0.0) for w in wide])
    downward = total([jnp.minimum(w, 0.0) for w in wide])
    up_count = total([(w > 0).astype(jnp.float32) for w in wide])
    down_count = total([(w < 0).astype(jnp.float32) for w in wide])
    balance = upward + downward
    upper = upward / jnp.maximum(up_count, 1.0)
    lower = downward / jnp.maximum(down_count, 1.0)
    agreed = jnp.where(balance > 0, upper, jnp.where(balance < 0, lower, 0.0))
    agreed = lax.all_gather(agreed, "task", axis=1, tiled=True)
    return base_weights.astype(jnp.float32) + agreed


def on_device(deltas, keep_blocks, base_weights):
    rows, width = deltas.shape[2:]
    square = lax.axis_size("task") == TASKS and STEPS * UNIT * LEVELS // STEPS < 2**15
    aligned = rows % (8 * TASKS) == 0 and BLOCK % rows == 0 and width % (16 * LANES) == 0
    if square and aligned:
        return square_body(deltas, keep_blocks, base_weights)
    return on_any_group(deltas, keep_blocks, base_weights)


def solution(mesh):
    in_specs = (P("task", None, "dp", "mp"), P("task", None, None), P(None, "dp", "mp"))
    out_specs = P(None, "dp", "mp")
    return jax.shard_map(
        on_device, mesh=mesh, in_specs=in_specs, out_specs=out_specs, check_vma=False
    )
```

```python
import functools
import math

import jax
import jax.numpy as jnp
from jax import lax
from jax.experimental import pallas as pl
from jax.experimental.pallas import tpu as pltpu
from jax.sharding import PartitionSpec as P


BLOCK = 128
STEPS = 64
LEVELS = 255
LANES = 512
TASKS = 4
UNIT = math.lcm(*range(1, TASKS + 1))
SLICES = (((1, 2), (3, 0)), ((1, 2, 3, 0),))
CUTS = (8, 6)
HBM = pl.BlockSpec(memory_space=pltpu.HBM)
VMEM = pl.BlockSpec(memory_space=pltpu.VMEM)


def params():
    return pltpu.CompilerParams(vmem_limit_bytes=8 * 2**20)


def hops(core, swapped):
    first = 1 + (core + swapped) % 2
    return 0, first, 3 - first, 3


def voter(hop):
    return lax.axis_index("task") ^ hops(lax.axis_index("mp"), 1)[hop]


def owner(hop):
    return lax.axis_index("task") ^ hops(lax.axis_index("mp"), 0)[hop]


def total(parts):
    out = parts[0]
    for part in parts[1:]:
        out = out + part
    return out


def over_columns(width, body):
    def step(j, _):
        body(pl.ds(pl.multiple_of(j * LANES, LANES), LANES))
        return 0

    lax.fori_loop(0, width // LANES, step, 0, unroll=2)


def split_kernel(start, which, keep_ref, deltas_ref, *rest):
    outs, (keep, sems, keep_sem) = rest[: len(which)], rest[len(which) :]
    projections, share, width = outs[0].shape
    block = 0
    if keep_ref.shape[0] > 1:
        block = lax.axis_index("dp") * (TASKS * share) // BLOCK
    flag = pltpu.make_async_copy(keep_ref, keep, keep_sem)
    copies = [
        pltpu.make_async_copy(
            deltas_ref.at[:, voter(hop), :, pl.ds(start, width)], out, sems.at[k]
        )
        for k, (hop, out) in enumerate(zip(which, outs))
    ]
    flag.start()
    for copy in copies:
        copy.start()
    flag.wait()
    for copy in copies:
        copy.wait()
    for p in range(projections):

        @pl.when(keep[block, p] == 0)
        def _(p=p):
            for out in outs:
                out[p] = jnp.zeros_like(out[p])


def split(keep, deltas, start, width, which):
    projections, _, share, _ = deltas.shape
    return pl.pallas_call(
        functools.partial(split_kernel, start, which),
        out_shape=[pltpu.VMEM((projections, share, width), deltas.dtype)] * len(which),
        in_specs=[HBM, HBM],
        out_specs=[VMEM] * len(which),
        scratch_shapes=[
            pltpu.SMEM(keep.shape, jnp.int32),
            pltpu.SemaphoreType.DMA((len(which),)),
            pltpu.SemaphoreType.DMA,
        ],
        compiler_params=params(),
    )(keep, deltas)


def fetch_kernel(source_ref, out_ref, sem):
    copy = pltpu.make_async_copy(source_ref, out_ref, sem)
    copy.start()
    copy.wait()


def fetch(x):
    return pl.pallas_call(
        fetch_kernel,
        out_shape=pltpu.VMEM(x.shape, x.dtype),
        in_specs=[HBM],
        out_specs=VMEM,
        scratch_shapes=[pltpu.SemaphoreType.DMA],
        compiler_params=params(),
        name="fetch",
    )(x)


def elect_kernel(*refs):
    *parts, code_ref = refs
    projections, _, width = code_ref.shape
    for p in range(projections):

        def body(at, p=p):
            wide = [part[p, :, at].astype(jnp.float32) for part in parts]
            balance = total(wide)
            sign = jnp.where(balance > 0, 1.0, jnp.where(balance < 0, -1.0, 0.0))
            toward = sign * STEPS
            agreeing = [jnp.maximum(w * toward, 0.0) for w in wide]
            count = total([jnp.minimum(a, 1.0) for a in agreeing])
            scale = jnp.full_like(count, UNIT)
            for c in range(2, TASKS + 1):
                scale = jnp.where(count == c, float(UNIT // c), scale)
            code = total(agreeing) * (scale * sign)
            code_ref[p, :, at] = code.astype(jnp.int32).astype(jnp.int16)

        over_columns(width, body)


def elect(parts):
    return pl.pallas_call(
        elect_kernel,
        out_shape=pltpu.VMEM(parts[0].shape, jnp.int16),
        in_specs=[VMEM] * TASKS,
        out_specs=VMEM,
        compiler_params=params(),
    )(*parts)


def merge_kernel(start, which, base_ref, *rest):
    codes, (out_ref, staged, sems) = rest[: len(which)], rest[-3:]
    projections, _, width = codes[0].shape
    copies = []
    for k, hop in enumerate(which):
        for p in range(projections):

            def body(at, k=k, hop=hop, p=p):
                there = pl.ds(pl.multiple_of(start + at.start, LANES), LANES)
                mean = codes[k][p, :, at].astype(jnp.int32).astype(jnp.float32)
                base = base_ref[p, owner(hop), :, there].astype(jnp.float32)
                staged[k, p, :, at] = base + mean * (1.0 / (STEPS * UNIT))

            over_columns(width, body)
            copies.append(
                pltpu.make_async_copy(
                    staged.at[k, p],
                    out_ref.at[p, owner(hop), :, pl.ds(start, width)],
                    sems.at[k, p],
                )
            )
            copies[-1].start()
    for copy in copies:
        copy.wait()


def merge(base, codes, start, which, so_far):
    extra, alias = ([], {}) if so_far is None else ([so_far], {1 + len(codes): 0})
    return pl.pallas_call(
        functools.partial(merge_kernel, start, which),
        out_shape=pltpu.HBM(base.shape, jnp.float32),
        in_specs=[VMEM] + [VMEM] * len(codes) + [HBM] * len(extra),
        out_specs=HBM,
        scratch_shapes=[
            pltpu.VMEM((len(codes), *codes[0].shape), jnp.float32),
            pltpu.SemaphoreType.DMA((len(codes), base.shape[0])),
        ],
        input_output_aliases=alias,
        compiler_params=params(),
    )(base, *codes, *extra)


def on_square(deltas, keep_blocks, base_weights):
    _, projections, rows, width = deltas.shape
    share, cores = rows // TASKS, lax.axis_size("mp")
    deltas = deltas.reshape(projections, TASKS, share, width)
    base = base_weights.reshape(projections, TASKS, share, width)
    keep = keep_blocks.transpose(0, 2, 1).reshape(-1, projections)
    keep, deltas, base = (
        pltpu.with_memory_space_constraint(a, pltpu.HBM) for a in (keep, deltas, base)
    )
    unit = width // sum(CUTS)
    chunks = [(unit * sum(CUTS[:i]), unit * cut) for i, cut in enumerate(CUTS)]

    def permute(x, hop, swapped=0):
        masks = [hops(c, swapped)[hop] for c in range(cores)]
        ends = [(i, i ^ mask, c) for i in range(TASKS) for c, mask in enumerate(masks)]
        pairs = [(i * cores + c, j * cores + c) for i, j, c in ends]
        return lax.ppermute(x, ("task", "mp"), pairs)

    parts = []
    for i, (start, size) in enumerate(chunks):
        held = []
        for which in SLICES[i]:
            held += split(keep, deltas, start, size, which)
        *others, own = held
        sent = [permute(x, k, 1) for k, x in enumerate(others, 1)]
        parts.append([own] + sent)
    base = fetch(base)
    code = []
    for part in parts:
        code.append(elect(part))
    first = [permute(c, 1) for c in code]
    second = [permute(c, 2) for c in code]
    across = [permute(c, 2) for c in first]
    merged = None
    for i, (start, _) in enumerate(chunks):
        near = [code[i], first[i], second[i]]
        merged = merge(base, near, start, (0, 1, 2), merged)
    for i, (start, _) in enumerate(chunks):
        merged = merge(base, [across[i]], start, (3,), merged)
    return merged.reshape(base_weights.shape)


def on_any_group(deltas, keep_blocks, base_weights):
    n = lax.axis_size("task")
    _, projections, rows, width = deltas.shape
    row_start = lax.axis_index("dp") * rows
    blocks = (row_start + jnp.arange(rows, dtype=jnp.int32)) // BLOCK
    keep = jnp.take(keep_blocks[0], blocks, axis=1)
    trimmed = jnp.where(keep[:, :, None] != 0, deltas[0], jnp.zeros((), deltas.dtype))
    split_rows = trimmed.reshape(projections, n, rows // n, width).swapaxes(0, 1)
    arrived = lax.all_to_all(split_rows, "task", split_axis=0, concat_axis=0, tiled=True)
    wide = [arrived[i].astype(jnp.float32) for i in range(n)]
    upward = total([jnp.maximum(w, 0.0) for w in wide])
    downward = total([jnp.minimum(w, 0.0) for w in wide])
    up_count = total([(w > 0).astype(jnp.float32) for w in wide])
    down_count = total([(w < 0).astype(jnp.float32) for w in wide])
    balance = upward + downward
    upper = upward / jnp.maximum(up_count, 1.0)
    lower = downward / jnp.maximum(down_count, 1.0)
    agreed = jnp.where(balance > 0, upper, jnp.where(balance < 0, lower, 0.0))
    agreed = lax.all_gather(agreed, "task", axis=1, tiled=True)
    return base_weights.astype(jnp.float32) + agreed


def on_device(deltas, keep_blocks, base_weights):
    rows, width = deltas.shape[2:]
    square = lax.axis_size("task") == TASKS and UNIT * LEVELS < 2**15
    aligned = rows % (8 * TASKS) == 0 and BLOCK % rows == 0 and width % (4 * LANES) == 0
    if square and aligned and width >= 8 * LANES:
        return on_square(deltas, keep_blocks, base_weights)
    return on_any_group(deltas, keep_blocks, base_weights)


def solution(mesh):
    in_specs = (P("task", None, "dp", "mp"), P("task", None, None), P(None, "dp", "mp"))
    out_specs = P(None, "dp", "mp")
    return jax.shard_map(
        on_device, mesh=mesh, in_specs=in_specs, out_specs=out_specs, check_vma=False
    )
```

```python
import functools
import math

import jax
import jax.numpy as jnp
from jax import lax
from jax.experimental import pallas as pl
from jax.experimental.pallas import tpu as pltpu
from jax.sharding import PartitionSpec as P


BLOCK = 128
STEPS = 64
LEVELS = 255
LANES = 512
TASKS = 4
UNIT = math.lcm(*range(1, TASKS + 1))
SLICES = (((1, 2), (3, 0)), ((1, 2, 3, 0),))
CUTS = (8, 6)
HBM = pl.BlockSpec(memory_space=pltpu.HBM)
VMEM = pl.BlockSpec(memory_space=pltpu.VMEM)


def params():
    return pltpu.CompilerParams(vmem_limit_bytes=8 * 2**20)


def hops(core, swapped):
    first = 1 + (core + swapped) % 2
    return 0, first, 3 - first, 3


def voter(hop):
    return lax.axis_index("task") ^ hops(lax.axis_index("mp"), 1)[hop]


def owner(hop):
    return lax.axis_index("task") ^ hops(lax.axis_index("mp"), 0)[hop]


def total(parts):
    out = parts[0]
    for part in parts[1:]:
        out = out + part
    return out


def over_columns(width, body):
    def step(j, _):
        body(pl.ds(pl.multiple_of(j * LANES, LANES), LANES))
        return 0

    lax.fori_loop(0, width // LANES, step, 0, unroll=2)


def split_kernel(start, which, keep_ref, deltas_ref, *rest):
    outs, (keep, sems, keep_sem) = rest[: len(which)], rest[len(which) :]
    projections, share, width = outs[0].shape
    block = 0
    if keep_ref.shape[0] > 1:
        block = lax.axis_index("dp") * (TASKS * share) // BLOCK
    flag = pltpu.make_async_copy(keep_ref, keep, keep_sem)
    copies = [
        pltpu.make_async_copy(
            deltas_ref.at[:, voter(hop), :, pl.ds(start, width)], out, sems.at[k]
        )
        for k, (hop, out) in enumerate(zip(which, outs))
    ]
    flag.start()
    for copy in copies:
        copy.start()
    flag.wait()
    for copy in copies:
        copy.wait()
    for p in range(projections):

        @pl.when(keep[block, p] == 0)
        def _(p=p):
            for out in outs:
                out[p] = jnp.zeros_like(out[p])


def split(keep, deltas, start, width, which):
    projections, _, share, _ = deltas.shape
    return pl.pallas_call(
        functools.partial(split_kernel, start, which),
        out_shape=[pltpu.VMEM((projections, share, width), deltas.dtype)] * len(which),
        in_specs=[HBM, HBM],
        out_specs=[VMEM] * len(which),
        scratch_shapes=[
            pltpu.SMEM(keep.shape, jnp.int32),
            pltpu.SemaphoreType.DMA((len(which),)),
            pltpu.SemaphoreType.DMA,
        ],
        compiler_params=params(),
    )(keep, deltas)


def fetch_kernel(source_ref, out_ref, sem):
    copy = pltpu.make_async_copy(source_ref, out_ref, sem)
    copy.start()
    copy.wait()


def fetch(x):
    return pl.pallas_call(
        fetch_kernel,
        out_shape=pltpu.VMEM(x.shape, x.dtype),
        in_specs=[HBM],
        out_specs=VMEM,
        scratch_shapes=[pltpu.SemaphoreType.DMA],
        compiler_params=params(),
        name="fetch",
    )(x)


def elect_kernel(*refs):
    *parts, code_ref = refs
    projections, _, width = code_ref.shape
    for p in range(projections):

        def body(at, p=p):
            wide = [part[p, :, at].astype(jnp.float32) for part in parts]
            balance = total(wide)
            sign = jnp.where(balance > 0, 1.0, jnp.where(balance < 0, -1.0, 0.0))
            toward = sign * STEPS
            agreeing = [jnp.maximum(w * toward, 0.0) for w in wide]
            count = total([jnp.minimum(a, 1.0) for a in agreeing])
            scale = jnp.full_like(count, UNIT)
            for c in range(2, TASKS + 1):
                scale = jnp.where(count == c, float(UNIT // c), scale)
            code = total(agreeing) * (scale * sign)
            code_ref[p, :, at] = code.astype(jnp.int32).astype(jnp.int16)

        over_columns(width, body)


def elect(parts):
    return pl.pallas_call(
        elect_kernel,
        out_shape=pltpu.VMEM(parts[0].shape, jnp.int16),
        in_specs=[VMEM] * TASKS,
        out_specs=VMEM,
        compiler_params=params(),
    )(*parts)


def merge_kernel(start, which, base_ref, *rest):
    codes, (out_ref, staged, sems) = rest[: len(which)], rest[-3:]
    projections, _, width = codes[0].shape
    copies = []
    for k, hop in enumerate(which):
        for p in range(projections):

            def body(at, k=k, hop=hop, p=p):
                there = pl.ds(pl.multiple_of(start + at.start, LANES), LANES)
                mean = codes[k][p, :, at].astype(jnp.int32).astype(jnp.float32)
                base = base_ref[p, owner(hop), :, there].astype(jnp.float32)
                staged[k, p, :, at] = base + mean * (1.0 / (STEPS * UNIT))

            over_columns(width, body)
            copies.append(
                pltpu.make_async_copy(
                    staged.at[k, p],
                    out_ref.at[p, owner(hop), :, pl.ds(start, width)],
                    sems.at[k, p],
                )
            )
            copies[-1].start()
    for copy in copies:
        copy.wait()


def merge(base, codes, start, which, so_far):
    extra, alias = ([], {}) if so_far is None else ([so_far], {1 + len(codes): 0})
    return pl.pallas_call(
        functools.partial(merge_kernel, start, which),
        out_shape=pltpu.HBM(base.shape, jnp.float32),
        in_specs=[VMEM] + [VMEM] * len(codes) + [HBM] * len(extra),
        out_specs=HBM,
        scratch_shapes=[
            pltpu.VMEM((len(codes), *codes[0].shape), jnp.float32),
            pltpu.SemaphoreType.DMA((len(codes), base.shape[0])),
        ],
        input_output_aliases=alias,
        compiler_params=params(),
    )(base, *codes, *extra)


def on_square(deltas, keep_blocks, base_weights):
    _, projections, rows, width = deltas.shape
    share, cores = rows // TASKS, lax.axis_size("mp")
    deltas = deltas.reshape(projections, TASKS, share, width)
    base = base_weights.reshape(projections, TASKS, share, width)
    keep = keep_blocks.transpose(0, 2, 1).reshape(-1, projections)
    keep, deltas, base = (
        pltpu.with_memory_space_constraint(a, pltpu.HBM) for a in (keep, deltas, base)
    )
    unit = width // sum(CUTS)
    chunks = [(unit * sum(CUTS[:i]), unit * cut) for i, cut in enumerate(CUTS)]

    def permute(x, hop, swapped=0):
        masks = [hops(c, swapped)[hop] for c in range(cores)]
        ends = [(i, i ^ mask, c) for i in range(TASKS) for c, mask in enumerate(masks)]
        pairs = [(i * cores + c, j * cores + c) for i, j, c in ends]
        return lax.ppermute(x, ("task", "mp"), pairs)

    parts = []
    for i, (start, size) in enumerate(chunks):
        held = []
        for which in SLICES[i]:
            held += split(keep, deltas, start, size, which)
        *others, own = held
        sent = [permute(x, k, 1) for k, x in enumerate(others, 1)]
        parts.append([own] + sent)
    base = fetch(base)
    code = []
    for part in parts:
        code.append(elect(part))
    first = [permute(c, 1) for c in code]
    second = [permute(c, 2) for c in code]
    across = [permute(c, 2) for c in first]
    merged = None
    for i, (start, _) in enumerate(chunks):
        near = [code[i], first[i], second[i]]
        merged = merge(base, near, start, (0, 1, 2), merged)
    for i, (start, _) in enumerate(chunks):
        merged = merge(base, [across[i]], start, (3,), merged)
    return merged.reshape(base_weights.shape)


def on_any_group(deltas, keep_blocks, base_weights):
    n = lax.axis_size("task")
    _, projections, rows, width = deltas.shape
    row_start = lax.axis_index("dp") * rows
    blocks = (row_start + jnp.arange(rows, dtype=jnp.int32)) // BLOCK
    keep = jnp.take(keep_blocks[0], blocks, axis=1)
    trimmed = jnp.where(keep[:, :, None] != 0, deltas[0], jnp.zeros((), deltas.dtype))
    split_rows = trimmed.reshape(projections, n, rows // n, width).swapaxes(0, 1)
    arrived = lax.all_to_all(split_rows, "task", split_axis=0, concat_axis=0, tiled=True)
    wide = [arrived[i].astype(jnp.float32) for i in range(n)]
    upward = total([jnp.maximum(w, 0.0) for w in wide])
    downward = total([jnp.minimum(w, 0.0) for w in wide])
    up_count = total([(w > 0).astype(jnp.float32) for w in wide])
    down_count = total([(w < 0).astype(jnp.float32) for w in wide])
    balance = upward + downward
    upper = upward / jnp.maximum(up_count, 1.0)
    lower = downward / jnp.maximum(down_count, 1.0)
    agreed = jnp.where(balance > 0, upper, jnp.where(balance < 0, lower, 0.0))
    agreed = lax.all_gather(agreed, "task", axis=1, tiled=True)
    return base_weights.astype(jnp.float32) + agreed


def on_device(deltas, keep_blocks, base_weights):
    rows, width = deltas.shape[2:]
    square = lax.axis_size("task") == TASKS and UNIT * LEVELS < 2**15
    whole_blocks = rows % (8 * TASKS) == 0 and BLOCK % rows == 0
    whole_columns = width % (sum(CUTS) * LANES) == 0
    if square and whole_blocks and whole_columns and deltas.shape[0] == 1:
        return on_square(deltas, keep_blocks, base_weights)
    return on_any_group(deltas, keep_blocks, base_weights)


def solution(mesh):
    in_specs = (P("task", None, "dp", "mp"), P("task", None, None), P(None, "dp", "mp"))
    out_specs = P(None, "dp", "mp")
    return jax.shard_map(
        on_device, mesh=mesh, in_specs=in_specs, out_specs=out_specs, check_vma=False
    )
```

```python
import functools
import math

import jax
import jax.numpy as jnp
from jax import lax
from jax.experimental import pallas as pl
from jax.experimental.pallas import tpu as pltpu
from jax.sharding import PartitionSpec as P


BLOCK = 128
STEPS = 64
LEVELS = 255
LANES = 512
TASKS = 4
UNIT = math.lcm(*range(1, TASKS + 1))
SLICES = (((1, 2), (3, 0)), ((1, 2, 3, 0),))
CUTS = (8, 6)
HBM = pl.BlockSpec(memory_space=pltpu.HBM)
VMEM = pl.BlockSpec(memory_space=pltpu.VMEM)


def params():
    return pltpu.CompilerParams(vmem_limit_bytes=8 * 2**20)


def hops(core, swapped):
    first = 1 + (core + swapped) % 2
    return 0, first, 3 - first, 3


def voter(hop):
    return lax.axis_index("task") ^ hops(lax.axis_index("mp"), 1)[hop]


def owner(hop):
    return lax.axis_index("task") ^ hops(lax.axis_index("mp"), 0)[hop]


def total(parts):
    out = parts[0]
    for part in parts[1:]:
        out = out + part
    return out


def over_columns(width, body, unroll=2):
    def step(j, _):
        body(pl.ds(pl.multiple_of(j * LANES, LANES), LANES))
        return 0

    lax.fori_loop(0, width // LANES, step, 0, unroll=min(unroll, width // LANES))


def split_kernel(start, which, keep_ref, deltas_ref, *rest):
    outs, (keep, sems, keep_sem) = rest[: len(which)], rest[len(which) :]
    projections, share, width = outs[0].shape
    block = 0
    if keep_ref.shape[0] > 1:
        block = lax.axis_index("dp") * (TASKS * share) // BLOCK
    flag = pltpu.make_async_copy(keep_ref, keep, keep_sem)
    copies = [
        pltpu.make_async_copy(
            deltas_ref.at[:, voter(hop), :, pl.ds(start, width)], out, sems.at[k]
        )
        for k, (hop, out) in enumerate(zip(which, outs))
    ]
    flag.start()
    for copy in copies:
        copy.start()
    flag.wait()
    for copy in copies:
        copy.wait()
    for p in range(projections):

        @pl.when(keep[block, p] == 0)
        def _(p=p):
            for out in outs:
                out[p] = jnp.zeros_like(out[p])


def split(keep, deltas, start, width, which):
    projections, _, share, _ = deltas.shape
    return pl.pallas_call(
        functools.partial(split_kernel, start, which),
        out_shape=[pltpu.VMEM((projections, share, width), deltas.dtype)] * len(which),
        in_specs=[HBM, HBM],
        out_specs=[VMEM] * len(which),
        scratch_shapes=[
            pltpu.SMEM(keep.shape, jnp.int32),
            pltpu.SemaphoreType.DMA((len(which),)),
            pltpu.SemaphoreType.DMA,
        ],
        compiler_params=params(),
    )(keep, deltas)


def fetch_kernel(source_ref, out_ref, sem):
    copy = pltpu.make_async_copy(source_ref, out_ref, sem)
    copy.start()
    copy.wait()


def fetch(x):
    return pl.pallas_call(
        fetch_kernel,
        out_shape=pltpu.VMEM(x.shape, x.dtype),
        in_specs=[HBM],
        out_specs=VMEM,
        scratch_shapes=[pltpu.SemaphoreType.DMA],
        compiler_params=params(),
        name="fetch",
    )(x)


def elect_kernel(*refs):
    *parts, code_ref = refs
    projections, _, width = code_ref.shape
    for p in range(projections):

        def body(at, p=p):
            wide = [part[p, :, at].astype(jnp.float32) for part in parts]
            balance = total(wide)
            sign = jnp.where(balance > 0, 1.0, jnp.where(balance < 0, -1.0, 0.0))
            toward = sign * STEPS
            agreeing = [jnp.maximum(w * toward, 0.0) for w in wide]
            count = total([jnp.minimum(a, 1.0) for a in agreeing])
            scale = jnp.full_like(count, UNIT)
            for c in range(2, TASKS + 1):
                scale = jnp.where(count == c, float(UNIT // c), scale)
            code = total(agreeing) * (scale * sign)
            code_ref[p, :, at] = code.astype(jnp.int32).astype(jnp.int16)

        over_columns(width, body)


def elect(parts):
    return pl.pallas_call(
        elect_kernel,
        out_shape=pltpu.VMEM(parts[0].shape, jnp.int16),
        in_specs=[VMEM] * TASKS,
        out_specs=VMEM,
        compiler_params=params(),
    )(*parts)


def merge_kernel(start, which, base_ref, *rest):
    codes, (out_ref, staged, sems) = rest[: len(which)], rest[-3:]
    projections, _, width = codes[0].shape
    copies = []
    for k, hop in enumerate(which):
        for p in range(projections):

            def body(at, k=k, hop=hop, p=p):
                there = pl.ds(pl.multiple_of(start + at.start, LANES), LANES)
                mean = codes[k][p, :, at].astype(jnp.int32).astype(jnp.float32)
                base = base_ref[p, owner(hop), :, there].astype(jnp.float32)
                staged[k, p, :, at] = base + mean * (1.0 / (STEPS * UNIT))

            over_columns(width, body, 12)
            copies.append(
                pltpu.make_async_copy(
                    staged.at[k, p],
                    out_ref.at[p, owner(hop), :, pl.ds(start, width)],
                    sems.at[k, p],
                )
            )
            copies[-1].start()
    for copy in copies:
        copy.wait()


def merge(base, codes, start, which, so_far):
    extra, alias = ([], {}) if so_far is None else ([so_far], {1 + len(codes): 0})
    return pl.pallas_call(
        functools.partial(merge_kernel, start, which),
        out_shape=pltpu.HBM(base.shape, jnp.float32),
        in_specs=[VMEM] + [VMEM] * len(codes) + [HBM] * len(extra),
        out_specs=HBM,
        scratch_shapes=[
            pltpu.VMEM((len(codes), *codes[0].shape), jnp.float32),
            pltpu.SemaphoreType.DMA((len(codes), base.shape[0])),
        ],
        input_output_aliases=alias,
        compiler_params=params(),
    )(base, *codes, *extra)


def on_square(deltas, keep_blocks, base_weights):
    _, projections, rows, width = deltas.shape
    share, cores = rows // TASKS, lax.axis_size("mp")
    deltas = deltas.reshape(projections, TASKS, share, width)
    base = base_weights.reshape(projections, TASKS, share, width)
    keep = keep_blocks.transpose(0, 2, 1).reshape(-1, projections)
    keep, deltas, base = (
        pltpu.with_memory_space_constraint(a, pltpu.HBM) for a in (keep, deltas, base)
    )
    unit = width // sum(CUTS)
    chunks = [(unit * sum(CUTS[:i]), unit * cut) for i, cut in enumerate(CUTS)]

    def permute(x, hop, swapped=0):
        masks = [hops(c, swapped)[hop] for c in range(cores)]
        ends = [(i, i ^ mask, c) for i in range(TASKS) for c, mask in enumerate(masks)]
        pairs = [(i * cores + c, j * cores + c) for i, j, c in ends]
        return lax.ppermute(x, ("task", "mp"), pairs)

    parts = []
    for i, (start, size) in enumerate(chunks):
        held = []
        for which in SLICES[i]:
            held += split(keep, deltas, start, size, which)
        *others, own = held
        sent = [permute(x, k, 1) for k, x in enumerate(others, 1)]
        parts.append([own] + sent)
    base = fetch(base)
    code = []
    for part in parts:
        code.append(elect(part))
    first = [permute(c, 1) for c in code]
    second = [permute(c, 2) for c in code]
    across = [permute(c, 2) for c in first]
    merged = None
    for i, (start, _) in enumerate(chunks):
        near = [code[i], first[i], second[i]]
        merged = merge(base, near, start, (0, 1, 2), merged)
    for i, (start, _) in enumerate(chunks):
        merged = merge(base, [across[i]], start, (3,), merged)
    return merged.reshape(base_weights.shape)


def on_any_group(deltas, keep_blocks, base_weights):
    n = lax.axis_size("task")
    _, projections, rows, width = deltas.shape
    row_start = lax.axis_index("dp") * rows
    blocks = (row_start + jnp.arange(rows, dtype=jnp.int32)) // BLOCK
    keep = jnp.take(keep_blocks[0], blocks, axis=1)
    trimmed = jnp.where(keep[:, :, None] != 0, deltas[0], jnp.zeros((), deltas.dtype))
    split_rows = trimmed.reshape(projections, n, rows // n, width).swapaxes(0, 1)
    arrived = lax.all_to_all(split_rows, "task", split_axis=0, concat_axis=0, tiled=True)
    wide = [arrived[i].astype(jnp.float32) for i in range(n)]
    upward = total([jnp.maximum(w, 0.0) for w in wide])
    downward = total([jnp.minimum(w, 0.0) for w in wide])
    up_count = total([(w > 0).astype(jnp.float32) for w in wide])
    down_count = total([(w < 0).astype(jnp.float32) for w in wide])
    balance = upward + downward
    upper = upward / jnp.maximum(up_count, 1.0)
    lower = downward / jnp.maximum(down_count, 1.0)
    agreed = jnp.where(balance > 0, upper, jnp.where(balance < 0, lower, 0.0))
    agreed = lax.all_gather(agreed, "task", axis=1, tiled=True)
    return base_weights.astype(jnp.float32) + agreed


def on_device(deltas, keep_blocks, base_weights):
    rows, width = deltas.shape[2:]
    square = lax.axis_size("task") == TASKS and UNIT * LEVELS < 2**15
    whole_blocks = rows % (8 * TASKS) == 0 and BLOCK % rows == 0
    whole_columns = width % (sum(CUTS) * LANES) == 0
    if square and whole_blocks and whole_columns and deltas.shape[0] == 1:
        return on_square(deltas, keep_blocks, base_weights)
    return on_any_group(deltas, keep_blocks, base_weights)


def solution(mesh):
    in_specs = (P("task", None, "dp", "mp"), P("task", None, None), P(None, "dp", "mp"))
    out_specs = P(None, "dp", "mp")
    return jax.shard_map(
        on_device, mesh=mesh, in_specs=in_specs, out_specs=out_specs, check_vma=False
    )
```

```python
import functools
import math

import jax
import jax.numpy as jnp
from jax import lax
from jax.experimental import pallas as pl
from jax.experimental.pallas import tpu as pltpu
from jax.sharding import PartitionSpec as P


BLOCK = 128
STEPS = 64
LEVELS = 255
LANES = 512
TASKS = 4
UNIT = math.lcm(*range(1, TASKS + 1))
SLICES = (((1, 2), (3, 0)), ((1, 2, 3, 0),))
ASIDE = (1024, 0)
CUTS = (8, 6)
HBM = pl.BlockSpec(memory_space=pltpu.HBM)
VMEM = pl.BlockSpec(memory_space=pltpu.VMEM)


def params():
    return pltpu.CompilerParams(vmem_limit_bytes=8 * 2**20)


def hops(core, swapped):
    first = 1 + (core + swapped) % 2
    return 0, first, 3 - first, 3


def voter(hop):
    return lax.axis_index("task") ^ hops(lax.axis_index("mp"), 1)[hop]


def owner(hop):
    return lax.axis_index("task") ^ hops(lax.axis_index("mp"), 0)[hop]


def total(parts):
    out = parts[0]
    for part in parts[1:]:
        out = out + part
    return out


def over_columns(width, body, unroll=2):
    def step(j, _):
        body(pl.ds(pl.multiple_of(j * LANES, LANES), LANES))
        return 0

    lax.fori_loop(0, width // LANES, step, 0, unroll=min(unroll, width // LANES))


def split_kernel(start, which, keep_ref, deltas_ref, *rest):
    outs, (keep, sems, keep_sem) = rest[: len(which)], rest[len(which) :]
    projections, share, width = outs[0].shape
    block = 0
    if keep_ref.shape[0] > 1:
        block = lax.axis_index("dp") * (TASKS * share) // BLOCK
    flag = pltpu.make_async_copy(keep_ref, keep, keep_sem)
    copies = [
        pltpu.make_async_copy(
            deltas_ref.at[:, voter(hop), :, pl.ds(start, width)], out, sems.at[k]
        )
        for k, (hop, out) in enumerate(zip(which, outs))
    ]
    flag.start()
    for copy in copies:
        copy.start()
    flag.wait()
    for copy in copies:
        copy.wait()
    for p in range(projections):

        @pl.when(keep[block, p] == 0)
        def _(p=p):
            for out in outs:
                out[p] = jnp.zeros_like(out[p])


def split(keep, deltas, start, width, which):
    projections, _, share, _ = deltas.shape
    return pl.pallas_call(
        functools.partial(split_kernel, start, which),
        out_shape=[pltpu.VMEM((projections, share, width), deltas.dtype)] * len(which),
        in_specs=[HBM, HBM],
        out_specs=[VMEM] * len(which),
        scratch_shapes=[
            pltpu.SMEM(keep.shape, jnp.int32),
            pltpu.SemaphoreType.DMA((len(which),)),
            pltpu.SemaphoreType.DMA,
        ],
        compiler_params=params(),
    )(keep, deltas)


def fetch_kernel(source_ref, out_ref, sem):
    copy = pltpu.make_async_copy(source_ref, out_ref, sem)
    copy.start()
    copy.wait()


def fetch(x):
    return pl.pallas_call(
        fetch_kernel,
        out_shape=pltpu.VMEM(x.shape, x.dtype),
        in_specs=[HBM],
        out_specs=VMEM,
        scratch_shapes=[pltpu.SemaphoreType.DMA],
        compiler_params=params(),
        name="fetch",
    )(x)


def elect_kernel(*refs):
    *parts, code_ref = refs
    projections, _, width = code_ref.shape
    for p in range(projections):

        def body(at, p=p):
            wide = [part[p, :, at].astype(jnp.float32) for part in parts]
            balance = total(wide)
            sign = jnp.where(balance > 0, 1.0, jnp.where(balance < 0, -1.0, 0.0))
            toward = sign * STEPS
            agreeing = [jnp.maximum(w * toward, 0.0) for w in wide]
            count = total([jnp.minimum(a, 1.0) for a in agreeing])
            scale = jnp.full_like(count, UNIT)
            for c in range(2, TASKS + 1):
                scale = jnp.where(count == c, float(UNIT // c), scale)
            code = total(agreeing) * (scale * sign)
            code_ref[p, :, at] = code.astype(jnp.int32).astype(jnp.int16)

        over_columns(width, body)


def elect(parts):
    return pl.pallas_call(
        elect_kernel,
        out_shape=pltpu.VMEM(parts[0].shape, jnp.int16),
        in_specs=[VMEM] * TASKS,
        out_specs=VMEM,
        compiler_params=params(),
    )(*parts)


def merge_kernel(places, base_ref, *rest):
    codes, (out_ref, staged, sems) = rest[: len(places)], rest[-3:]
    copies = []
    for k, (start, hop) in enumerate(places):
        projections, _, width = codes[k].shape
        for p in range(projections):

            def body(at, k=k, start=start, hop=hop, p=p):
                there = pl.ds(pl.multiple_of(start + at.start, LANES), LANES)
                mean = codes[k][p, :, at].astype(jnp.int32).astype(jnp.float32)
                base = base_ref[p, owner(hop), :, there].astype(jnp.float32)
                staged[k, p, :, at] = base + mean * (1.0 / (STEPS * UNIT))

            over_columns(width, body, 4)
            copies.append(
                pltpu.make_async_copy(
                    staged.at[k, p, :, pl.ds(0, width)],
                    out_ref.at[p, owner(hop), :, pl.ds(start, width)],
                    sems.at[k, p],
                )
            )
            copies[-1].start()
    for copy in copies:
        copy.wait()


def merge(base, pieces, so_far):
    codes = [piece[0] for piece in pieces]
    places = tuple(piece[1:] for piece in pieces)
    width = max(code.shape[-1] for code in codes)
    extra, alias = ([], {}) if so_far is None else ([so_far], {1 + len(codes): 0})
    return pl.pallas_call(
        functools.partial(merge_kernel, places),
        out_shape=pltpu.HBM(base.shape, jnp.float32),
        in_specs=[VMEM] + [VMEM] * len(codes) + [HBM] * len(extra),
        out_specs=HBM,
        scratch_shapes=[
            pltpu.VMEM((len(codes), *codes[0].shape[:-1], width), jnp.float32),
            pltpu.SemaphoreType.DMA((len(codes), base.shape[0])),
        ],
        input_output_aliases=alias,
        compiler_params=params(),
    )(base, *codes, *extra)


def on_square(deltas, keep_blocks, base_weights):
    _, projections, rows, width = deltas.shape
    share, cores = rows // TASKS, lax.axis_size("mp")
    deltas = deltas.reshape(projections, TASKS, share, width)
    base = base_weights.reshape(projections, TASKS, share, width)
    keep = keep_blocks.transpose(0, 2, 1).reshape(-1, projections)
    keep, deltas, base = (
        pltpu.with_memory_space_constraint(a, pltpu.HBM) for a in (keep, deltas, base)
    )
    unit = width // sum(CUTS)
    chunks = [(unit * sum(CUTS[:i]), unit * cut) for i, cut in enumerate(CUTS)]

    def permute(x, hop, swapped=0):
        masks = [hops(c, swapped)[hop] for c in range(cores)]
        ends = [(i, i ^ mask, c) for i in range(TASKS) for c, mask in enumerate(masks)]
        pairs = [(i * cores + c, j * cores + c) for i, j, c in ends]
        return lax.ppermute(x, ("task", "mp"), pairs)

    parts = []
    for i, (start, size) in enumerate(chunks):
        held = []
        for which in SLICES[i]:
            held += split(keep, deltas, start, size, which)
        *others, own = held
        sent = [permute(x, k, 1) for k, x in enumerate(others, 1)]
        parts.append([own] + sent)
    base = fetch(base)
    code = []
    for part in parts:
        code.append(elect(part))
    first = [permute(c, 1) for c in code]
    second = [permute(c, 2) for c in code]
    across = []
    for i, (start, size) in enumerate(chunks):
        keep_to = size - ASIDE[i]
        main = permute(first[i][:, :, :keep_to], 2)
        across.append([(main, start, 3)])
        if ASIDE[i]:
            even = lax.axis_index("mp") % 2 == 0
            vertical = jnp.where(even, second[i][:, :, keep_to:], first[i][:, :, keep_to:])
            pairs = [(d, d ^ cores) for d in range(TASKS * cores)]
            rest = lax.ppermute(vertical, ("task", "mp"), pairs)
            across[i].append((rest, start + keep_to, 3))
    merged = None
    for i, (start, _) in enumerate(chunks):
        near = [(code[i], start, 0), (first[i], start, 1), (second[i], start, 2)]
        merged = merge(base, near, merged)
    for i in range(len(chunks)):
        merged = merge(base, across[i], merged)
    return merged.reshape(base_weights.shape)


def on_any_group(deltas, keep_blocks, base_weights):
    n = lax.axis_size("task")
    _, projections, rows, width = deltas.shape
    row_start = lax.axis_index("dp") * rows
    blocks = (row_start + jnp.arange(rows, dtype=jnp.int32)) // BLOCK
    keep = jnp.take(keep_blocks[0], blocks, axis=1)
    trimmed = jnp.where(keep[:, :, None] != 0, deltas[0], jnp.zeros((), deltas.dtype))
    split_rows = trimmed.reshape(projections, n, rows // n, width).swapaxes(0, 1)
    arrived = lax.all_to_all(split_rows, "task", split_axis=0, concat_axis=0, tiled=True)
    wide = [arrived[i].astype(jnp.float32) for i in range(n)]
    upward = total([jnp.maximum(w, 0.0) for w in wide])
    downward = total([jnp.minimum(w, 0.0) for w in wide])
    up_count = total([(w > 0).astype(jnp.float32) for w in wide])
    down_count = total([(w < 0).astype(jnp.float32) for w in wide])
    balance = upward + downward
    upper = upward / jnp.maximum(up_count, 1.0)
    lower = downward / jnp.maximum(down_count, 1.0)
    agreed = jnp.where(balance > 0, upper, jnp.where(balance < 0, lower, 0.0))
    agreed = lax.all_gather(agreed, "task", axis=1, tiled=True)
    return base_weights.astype(jnp.float32) + agreed


def on_device(deltas, keep_blocks, base_weights):
    rows, width = deltas.shape[2:]
    square = lax.axis_size("task") == TASKS and UNIT * LEVELS < 2**15
    whole_blocks = rows % (8 * TASKS) == 0 and BLOCK % rows == 0
    whole_columns = width % (sum(CUTS) * LANES) == 0
    if square and whole_blocks and whole_columns and deltas.shape[0] == 1:
        return on_square(deltas, keep_blocks, base_weights)
    return on_any_group(deltas, keep_blocks, base_weights)


def solution(mesh):
    in_specs = (P("task", None, "dp", "mp"), P("task", None, None), P(None, "dp", "mp"))
    out_specs = P(None, "dp", "mp")
    return jax.shard_map(
        on_device, mesh=mesh, in_specs=in_specs, out_specs=out_specs, check_vma=False
    )
```

```python
import functools
import math

import jax
import jax.numpy as jnp
from jax import lax
from jax.experimental import pallas as pl
from jax.experimental.pallas import tpu as pltpu
from jax.sharding import PartitionSpec as P


BLOCK = 128
STEPS = 64
LEVELS = 255
XCH = (0, 0)
GAT = (1, 0)
LANES = 512
TASKS = 4
UNIT = math.lcm(*range(1, TASKS + 1))
SLICES = (((1, 2), (3, 0)), ((1, 2, 3, 0),))
CUTS = (8, 6)
HBM = pl.BlockSpec(memory_space=pltpu.HBM)
VMEM = pl.BlockSpec(memory_space=pltpu.VMEM)


def params():
    return pltpu.CompilerParams(vmem_limit_bytes=8 * 2**20)


def hops(core, swapped):
    first = 1 + (core + swapped) % 2
    return 0, first, 3 - first, 3


def voter(hop, chunk):
    return lax.axis_index("task") ^ hops(lax.axis_index("mp"), XCH[chunk])[hop]


def owner(hop, chunk):
    return lax.axis_index("task") ^ hops(lax.axis_index("mp"), GAT[chunk])[hop]


def total(parts):
    out = parts[0]
    for part in parts[1:]:
        out = out + part
    return out


def over_columns(width, body):
    def step(j, _):
        body(pl.ds(pl.multiple_of(j * LANES, LANES), LANES))
        return 0

    lax.fori_loop(0, width // LANES, step, 0, unroll=2)


def split_kernel(start, which, keep_ref, deltas_ref, *rest):
    outs, (keep, sems, keep_sem) = rest[: len(which)], rest[len(which) :]
    projections, share, width = outs[0].shape
    block = 0
    if keep_ref.shape[0] > 1:
        block = lax.axis_index("dp") * (TASKS * share) // BLOCK
    flag = pltpu.make_async_copy(keep_ref, keep, keep_sem)
    copies = [
        pltpu.make_async_copy(
            deltas_ref.at[:, voter(hop, 0 if start == 0 else 1), :, pl.ds(start, width)], out, sems.at[k]
        )
        for k, (hop, out) in enumerate(zip(which, outs))
    ]
    flag.start()
    for copy in copies:
        copy.start()
    flag.wait()
    for copy in copies:
        copy.wait()
    for p in range(projections):

        @pl.when(keep[block, p] == 0)
        def _(p=p):
            for out in outs:
                out[p] = jnp.zeros_like(out[p])


def split(keep, deltas, start, width, which):
    projections, _, share, _ = deltas.shape
    return pl.pallas_call(
        functools.partial(split_kernel, start, which),
        out_shape=[pltpu.VMEM((projections, share, width), deltas.dtype)] * len(which),
        in_specs=[HBM, HBM],
        out_specs=[VMEM] * len(which),
        scratch_shapes=[
            pltpu.SMEM(keep.shape, jnp.int32),
            pltpu.SemaphoreType.DMA((len(which),)),
            pltpu.SemaphoreType.DMA,
        ],
        compiler_params=params(),
    )(keep, deltas)


def fetch_kernel(source_ref, out_ref, sem):
    copy = pltpu.make_async_copy(source_ref, out_ref, sem)
    copy.start()
    copy.wait()


def fetch(x):
    return pl.pallas_call(
        fetch_kernel,
        out_shape=pltpu.VMEM(x.shape, x.dtype),
        in_specs=[HBM],
        out_specs=VMEM,
        scratch_shapes=[pltpu.SemaphoreType.DMA],
        compiler_params=params(),
        name="fetch",
    )(x)


def elect_kernel(*refs):
    *parts, code_ref = refs
    projections, _, width = code_ref.shape
    for p in range(projections):

        def body(at, p=p):
            wide = [part[p, :, at].astype(jnp.float32) for part in parts]
            balance = total(wide)
            sign = jnp.where(balance > 0, 1.0, jnp.where(balance < 0, -1.0, 0.0))
            toward = sign * STEPS
            agreeing = [jnp.maximum(w * toward, 0.0) for w in wide]
            count = total([jnp.minimum(a, 1.0) for a in agreeing])
            scale = jnp.full_like(count, UNIT)
            for c in range(2, TASKS + 1):
                scale = jnp.where(count == c, float(UNIT // c), scale)
            code = total(agreeing) * (scale * sign)
            code_ref[p, :, at] = code.astype(jnp.int32).astype(jnp.int16)

        over_columns(width, body)


def elect(parts):
    return pl.pallas_call(
        elect_kernel,
        out_shape=pltpu.VMEM(parts[0].shape, jnp.int16),
        in_specs=[VMEM] * TASKS,
        out_specs=VMEM,
        compiler_params=params(),
    )(*parts)


def merge_kernel(start, which, base_ref, *rest):
    codes, (out_ref, staged, sems) = rest[: len(which)], rest[-3:]
    projections, _, width = codes[0].shape
    copies = []
    for k, hop in enumerate(which):
        for p in range(projections):

            def body(at, k=k, hop=hop, p=p):
                there = pl.ds(pl.multiple_of(start + at.start, LANES), LANES)
                mean = codes[k][p, :, at].astype(jnp.int32).astype(jnp.float32)
                base = base_ref[p, owner(hop, 0 if start == 0 else 1), :, there].astype(jnp.float32)
                staged[k, p, :, at] = base + mean * (1.0 / (STEPS * UNIT))

            over_columns(width, body)
            copies.append(
                pltpu.make_async_copy(
                    staged.at[k, p],
                    out_ref.at[p, owner(hop, 0 if start == 0 else 1), :, pl.ds(start, width)],
                    sems.at[k, p],
                )
            )
            copies[-1].start()
    for copy in copies:
        copy.wait()


def merge(base, codes, start, which, so_far):
    extra, alias = ([], {}) if so_far is None else ([so_far], {1 + len(codes): 0})
    return pl.pallas_call(
        functools.partial(merge_kernel, start, which),
        out_shape=pltpu.HBM(base.shape, jnp.float32),
        in_specs=[VMEM] + [VMEM] * len(codes) + [HBM] * len(extra),
        out_specs=HBM,
        scratch_shapes=[
            pltpu.VMEM((len(codes), *codes[0].shape), jnp.float32),
            pltpu.SemaphoreType.DMA((len(codes), base.shape[0])),
        ],
        input_output_aliases=alias,
        compiler_params=params(),
    )(base, *codes, *extra)


def on_square(deltas, keep_blocks, base_weights):
    _, projections, rows, width = deltas.shape
    share, cores = rows // TASKS, lax.axis_size("mp")
    deltas = deltas.reshape(projections, TASKS, share, width)
    base = base_weights.reshape(projections, TASKS, share, width)
    keep = keep_blocks.transpose(0, 2, 1).reshape(-1, projections)
    keep, deltas, base = (
        pltpu.with_memory_space_constraint(a, pltpu.HBM) for a in (keep, deltas, base)
    )
    unit = width // sum(CUTS)
    chunks = [(unit * sum(CUTS[:i]), unit * cut) for i, cut in enumerate(CUTS)]

    def permute(x, hop, swapped=0):
        masks = [hops(c, swapped)[hop] for c in range(cores)]
        ends = [(i, i ^ mask, c) for i in range(TASKS) for c, mask in enumerate(masks)]
        pairs = [(i * cores + c, j * cores + c) for i, j, c in ends]
        return lax.ppermute(x, ("task", "mp"), pairs)

    parts = []
    for i, (start, size) in enumerate(chunks):
        held = []
        for which in SLICES[i]:
            held += split(keep, deltas, start, size, which)
        *others, own = held
        sent = [permute(x, k, XCH[i]) for k, x in enumerate(others, 1)]
        parts.append([own] + sent)
    base = fetch(base)
    code = []
    for part in parts:
        code.append(elect(part))
    first = [permute(c, 1, GAT[i]) for i, c in enumerate(code)]
    second = [permute(c, 2, GAT[i]) for i, c in enumerate(code)]
    across = [permute(c, 2, GAT[i]) for i, c in enumerate(first)]
    merged = None
    for i, (start, _) in enumerate(chunks):
        near = [code[i], first[i], second[i]]
        merged = merge(base, near, start, (0, 1, 2), merged)
    for i, (start, _) in enumerate(chunks):
        merged = merge(base, [across[i]], start, (3,), merged)
    return merged.reshape(base_weights.shape)


def on_any_group(deltas, keep_blocks, base_weights):
    n = lax.axis_size("task")
    _, projections, rows, width = deltas.shape
    row_start = lax.axis_index("dp") * rows
    blocks = (row_start + jnp.arange(rows, dtype=jnp.int32)) // BLOCK
    keep = jnp.take(keep_blocks[0], blocks, axis=1)
    trimmed = jnp.where(keep[:, :, None] != 0, deltas[0], jnp.zeros((), deltas.dtype))
    split_rows = trimmed.reshape(projections, n, rows // n, width).swapaxes(0, 1)
    arrived = lax.all_to_all(split_rows, "task", split_axis=0, concat_axis=0, tiled=True)
    wide = [arrived[i].astype(jnp.float32) for i in range(n)]
    upward = total([jnp.maximum(w, 0.0) for w in wide])
    downward = total([jnp.minimum(w, 0.0) for w in wide])
    up_count = total([(w > 0).astype(jnp.float32) for w in wide])
    down_count = total([(w < 0).astype(jnp.float32) for w in wide])
    balance = upward + downward
    upper = upward / jnp.maximum(up_count, 1.0)
    lower = downward / jnp.maximum(down_count, 1.0)
    agreed = jnp.where(balance > 0, upper, jnp.where(balance < 0, lower, 0.0))
    agreed = lax.all_gather(agreed, "task", axis=1, tiled=True)
    return base_weights.astype(jnp.float32) + agreed


def on_device(deltas, keep_blocks, base_weights):
    rows, width = deltas.shape[2:]
    square = lax.axis_size("task") == TASKS and UNIT * LEVELS < 2**15
    whole_blocks = rows % (8 * TASKS) == 0 and BLOCK % rows == 0
    whole_columns = width % (sum(CUTS) * LANES) == 0
    if square and whole_blocks and whole_columns and deltas.shape[0] == 1:
        return on_square(deltas, keep_blocks, base_weights)
    return on_any_group(deltas, keep_blocks, base_weights)


def solution(mesh):
    in_specs = (P("task", None, "dp", "mp"), P("task", None, None), P(None, "dp", "mp"))
    out_specs = P(None, "dp", "mp")
    return jax.shard_map(
        on_device, mesh=mesh, in_specs=in_specs, out_specs=out_specs, check_vma=False
    )
```
